32 devices in a mesh: replica: 16 (over z, x, core), spatial: 2 (over y).
Axes of the slice: x: 2, y: 2, z: 4, core: 2. Of those that a mesh axis runs over, the one named last changes fastest.
Arguments:
- grads: bfloat16 [16, 2, 852992], P('replica', 'spatial'), may hold values from -6 to 6
- master: float32 [852992], P(('replica', 'spatial')), may hold values from -0.06 to 0.06
- velocity: float32 [852992], P(('replica', 'spatial')), may hold values from -0.3 to 0.3
- layer_offsets: int32 [6], replicated, may hold values from 0 to 852736, as said below
- layer_sizes: int32 [6], replicated, may hold values from 256 to 589824
- lars_skip: int32 [6], replicated, may hold values from 0 to 1
Outputs:
- new_weights: bfloat16 [852992], replicated
- new_master: float32 [852992], P(('replica', 'spatial'))
- new_velocity: float32 [852992], P(('replica', 'spatial'))
The draws below stay inside these ranges and needn't reach their ends.
Inputs may be any that keep to these rules, and one draw needn't show every extreme that they name: layer_offsets, layer_sizes and lars_skip describe the six tensors (a 256 x 1024 convolution, a 256 x 256 x 9 convolution, and two gains and two shifts of 256 entries) laid end to end in some order without gaps, the last of them always a gain or a shift; lars_skip is 1 exactly for the gains and shifts.
All inputs are finite; a program needn't handle non-finite values.
Results may differ from the reference program's by a relative error of at most 0.001.
Values may be sent and summed in bfloat16 or wider, within the bound.
A program may use at most 64 MiB of HBM per device.

```python
import jax
import jax.numpy as jnp
from jax import lax

CIN = 1024
MID = 256
KSQ = 9
LAYERS = 6
PARAMS = 852992
N_REPLICA = 16
N_SPATIAL = 2


def layout_tables(key):
    scores = jax.random.permutation(jax.random.fold_in(key, 71), LAYERS).astype(jnp.int32)
    small_list = jnp.array([1, 2, 4, 5], jnp.int32)
    pick = jax.random.randint(jax.random.fold_in(key, 73), (), 0, 4)
    chosen = small_list[pick]
    scores = jnp.where(jnp.arange(LAYERS, dtype=jnp.int32) == chosen, LAYERS, scores)
    order = jnp.argsort(scores, stable=True)
    base_sizes = jnp.array([MID * CIN, MID, MID, MID * MID * KSQ, MID, MID], jnp.int32)
    base_skip = jnp.array([0, 1, 1, 0, 1, 1], jnp.int32)
    sizes = base_sizes[order]
    offsets = jnp.cumsum(sizes) - sizes
    return (offsets.astype(jnp.int32), sizes.astype(jnp.int32), base_skip[order])


def draw_layer_offsets(key, part):
    return layout_tables(key)[0]


def draw_layer_sizes(key, part):
    return layout_tables(key)[1]


def draw_lars_skip(key, part):
    return layout_tables(key)[2]


def raised(values, rng, source, target, blocks, factor):
    owner, partner = [(jnp.arange(values.shape[dim]) // (values.shape[dim] // blocks)).reshape([-1 if axis == dim else 1 for axis in range(values.ndim)]) for dim in (source, target)]
    chosen = jax.random.permutation(rng, blocks)[partner]
    strong = (owner == chosen) | (owner == (partner + blocks // 2) % blocks)
    return jnp.where(strong, factor * values, values)


def levels(stream_key, extent, split, smallest, high):
    loudness, own = 1.0, jax.random.fold_in(stream_key, 6)
    for axis_at, blocks in split:
        heights = jnp.exp(jax.random.uniform(jax.random.fold_in(own, axis_at), (blocks,), jnp.float32, smallest / len(split), high / len(split)))
        loudness = loudness * jnp.repeat(heights, extent[axis_at] // blocks).reshape([-1 if axis == axis_at else 1 for axis in range(len(extent))])
    return loudness


def gaussian(stream_key, extent, scale, limit, cuts=(), held_as=jnp.bfloat16):
    values = jax.random.normal(stream_key, extent, jnp.float32) * scale
    if len(cuts) > 0:
        values = levels(stream_key, extent, cuts, -0.22, 0.18) * values
    return jnp.clip(values, min=-limit, max=limit).astype(held_as)


def gaussian_with(key, shape, scale, bound, pieces, heavy, kind=jnp.bfloat16):
    values = scale * jax.random.normal(key, shape, jnp.float32)
    if pieces:
        values = values * levels(key, shape, pieces, -0.22, 0.18)
    return jnp.clip(raised(values, jax.random.fold_in(key, 3), *heavy), -bound, bound).astype(kind)


def setup_inputs(seed: int = 0) -> dict:
    keys = jax.random.split(jax.random.key(seed), 7)
    grads = gaussian_with(keys[0], (N_REPLICA, N_SPATIAL, PARAMS), 1.0, 6.0, ((0, 16), (1, 2)), (0, 2, 16, 2.0))
    master = jnp.clip(jax.random.uniform(keys[1], (PARAMS,), jnp.float32, -0.06, 0.06) * levels(keys[1], (PARAMS,), ((0, 32),), -0.4, 0.0), -0.06, 0.06)
    velocity = gaussian(keys[2], (PARAMS,), 0.05, 0.3, ((0, 32),), jnp.float32)
    layer_offsets = draw_layer_offsets(jax.random.fold_in(keys[6], 71), 0)
    layer_sizes = draw_layer_sizes(jax.random.fold_in(keys[6], 71), 0)
    lars_skip = draw_lars_skip(jax.random.fold_in(keys[6], 71), 0)
    return dict(grads=grads, master=master, velocity=velocity, layer_offsets=layer_offsets, layer_sizes=layer_sizes, lars_skip=lars_skip)


def reference(grads, master, velocity, layer_offsets, layer_sizes, lars_skip):
    grad = lax.optimization_barrier(jnp.sum(grads.astype(jnp.float32), axis=(0, 1))) / (N_REPLICA * N_SPATIAL)
    position = jnp.arange(PARAMS, dtype=jnp.int32)
    inside = (position[None, :] >= layer_offsets[:, None]) & (position[None, :] < (layer_offsets + layer_sizes)[:, None])
    onehot = inside.astype(jnp.float32)
    wsq = jnp.dot(onehot, master * master, precision=lax.Precision.HIGHEST)
    gsq = jnp.dot(onehot, grad * grad, precision=lax.Precision.HIGHEST)
    wnorm = jnp.sqrt(wsq)
    gnorm = jnp.sqrt(gsq)
    skipped = lars_skip.astype(jnp.float32)
    ratio = 0.02 * wnorm / (gnorm + 0.001 * wnorm + 1e-06)
    trust = skipped + (1.0 - skipped) * ratio
    decay = (1.0 - skipped) * 0.001
    trust_pos = jnp.dot(trust, onehot, precision=lax.Precision.HIGHEST)
    decay_pos = jnp.dot(decay, onehot, precision=lax.Precision.HIGHEST)
    new_velocity = 0.9 * velocity + 8.0 * trust_pos * (grad + decay_pos * master)
    new_master = master - new_velocity
    return (new_master.astype(jnp.bfloat16), new_master, new_velocity)
```

```python
import functools
import math

import jax
import jax.numpy as jnp
from jax import lax
from jax.experimental import pallas as pl
from jax.experimental.pallas import tpu as pltpu
from jax.sharding import PartitionSpec as P

MESH = pl.DeviceIdType.MESH
TILE = 1024


def kernel(
    plan,
    grads_ref,
    m_ref,
    v_ref,
    offsets_ref,
    sizes_ref,
    skip_ref,
    out_ref,
    nm_ref,
    nv_ref,
    gin,
    packed,
    recv1,
    part,
    recv2,
    mv,
    halo,
    grad_buf,
    wrow,
    stats,
    ags,
    nmw,
    nvw,
    in_sem,
    send1,
    got1,
    send2,
    got2,
    halo_sem,
    send3,
    got3,
    send4,
    got4,
    out_sem,
):
    n_out, n_a, n_spa, shard, step, span, layers = plan
    plane = n_a * 2 * n_spa
    n = n_out * plane
    chunk = (plane - 1) * step + span
    rows = span * 8
    r = lax.axis_index("replica")
    s = lax.axis_index("spatial")
    d = r * n_spa + s
    z = d // plane
    p = d % plane
    a = p // (2 * n_spa)
    c = (p // n_spa) % 2
    base = d * (step * TILE)
    off = d * (shard - step * TILE)

    def dev(flat):
        return (flat // n_spa, flat % n_spa)

    barrier = pltpu.get_barrier_semaphore()

    @pl.loop(1, n)
    def _(q):
        pl.semaphore_signal(barrier, inc=1, device_id=dev((d + q) % n), device_id_type=MESH)

    def load(zt):
        start = pl.multiple_of(zt * (plane * step * TILE), TILE)
        return pltpu.make_async_copy(
            grads_ref.at[0, :, pl.ds(start, chunk * TILE)], gin.at[zt], in_sem.at[zt]
        )

    for k in range(1, n_out + 1):
        load((z + k) % n_out).start()

    group = max(g for g in range(1, 33) if chunk % g == 0)

    def pack(zt):
        load(zt).wait()

        @pl.loop(0, chunk // group)
        def _(i):
            at = pl.multiple_of(i * (group * TILE), group * TILE)
            v = gin[zt, :, pl.ds(at, group * TILE)].astype(jnp.float32)
            packed[zt, pl.ds(i * group, group)] = v.reshape(group, 8, 128).astype(jnp.bfloat16)

    def copy1(zt, src, dst):
        return pltpu.make_async_remote_copy(
            src_ref=packed.at[zt, pl.ds(dst * step, span)],
            dst_ref=recv1.at[zt, src],
            send_sem=send1.at[zt, dst],
            recv_sem=got1.at[zt, src],
            device_id=dev(z * plane + dst),
            device_id_type=MESH,
        )

    for k in range(1, n_out + 1):
        zt = (z + k) % n_out
        pack(zt)
        if k == 1:
            pl.semaphore_wait(barrier, n - 1)

        @pl.loop(1, plane)
        def _(q):
            copy1(zt, p, (p + q) % plane).start()

    lane = lax.broadcasted_iota(jnp.int32, (rows, 128), 1)
    shift_l = off % 128
    shift_r = off // 128
    for j, ref in enumerate((m_ref, v_ref)):
        x = pltpu.roll(ref[...], shift_l, 1)
        x = jnp.where(lane < shift_l, pltpu.roll(x, 1, 0), x)
        x = pltpu.roll(x, shift_r, 0)
        mv[:, j] = x.reshape(span, 8, 128)
    halo_copy = pltpu.make_async_remote_copy(
        src_ref=mv.at[span - 1],
        dst_ref=halo,
        send_sem=halo_sem.at[0],
        recv_sem=halo_sem.at[1],
        device_id=dev((d + 1) % n),
        device_id_type=MESH,
    )
    halo_copy.start()

    place = lax.broadcasted_iota(jnp.int32, (8, 128), 0) * 128 + lax.broadcasted_iota(
        jnp.int32, (8, 128), 1
    )
    low = [offsets_ref[l] - base for l in range(layers)]
    high = [offsets_ref[l] + sizes_ref[l] - base for l in range(layers)]
    own_low = [jnp.maximum(x, off) for x in low]
    own_high = [jnp.minimum(x, off + shard) for x in high]
    lane1 = lax.broadcasted_iota(jnp.int32, (1, 128), 1)

    def squares(value, first):
        def add(t, accs):
            pos = place + t * TILE
            x = value(t)
            x = x * x
            return tuple(
                acc + jnp.where((pos >= lo) & (pos < hi), x, 0.0)
                for acc, lo, hi in zip(accs, own_low, own_high)
            )

        accs = lax.fori_loop(
            0, span, add, tuple(jnp.zeros((8, 128), jnp.float32) for _ in range(layers))
        )
        row = jnp.zeros((1, 128), jnp.float32)
        for l, acc in enumerate(accs):
            row = jnp.where(lane1 == first + l, jnp.sum(acc, axis=(0, 1), keepdims=True), row)
        return row

    wrow[...] = squares(lambda t: mv[t, 0], 0)

    def copy2(zt, src):
        return pltpu.make_async_remote_copy(
            src_ref=part.at[zt],
            dst_ref=recv2.at[src],
            send_sem=send2.at[zt],
            recv_sem=got2.at[src],
            device_id=dev(zt * plane + p),
            device_id_type=MESH,
        )

    for k in range(1, n_out + 1):
        zt = (z + k) % n_out

        @pl.loop(1, plane)
        def _(q):
            copy1(zt, (p + q) % plane, p).wait_recv()

        @pl.loop(0, span)
        def _(t):
            acc = packed[zt, p * step + t].astype(jnp.float32)
            for q in range(1, plane):
                acc = acc + recv1[zt, (p + q) % plane, t].astype(jnp.float32)
            part[zt, t] = acc

        if k < n_out:
            copy2(zt, z).start()

    halo_copy.wait()
    for j in range(2):
        mv[0, j] = jnp.where(place < off, halo[j], mv[0, j])

    @pl.loop(1, n_out)
    def _(k):
        copy2(z, (z + k) % n_out).wait_recv()

    @pl.loop(0, span)
    def _(t):
        acc = part[z, t]
        for k in range(1, n_out):
            acc = acc + recv2[(z + k) % n_out, t]
        grad_buf[t] = acc / n

    stats[d] = squares(lambda t: grad_buf[t], layers) + wrow[...]

    def copy3(src, dst):
        return pltpu.make_async_remote_copy(
            src_ref=stats.at[src],
            dst_ref=stats.at[src],
            send_sem=send3.at[dst],
            recv_sem=got3.at[src],
            device_id=dev(dst),
            device_id_type=MESH,
        )

    @pl.loop(1, n)
    def _(q):
        copy3(d, (d + q) % n).start()

    @pl.loop(1, n)
    def _(q):
        copy3((d + q) % n, d).wait_recv()

    total = jnp.sum(stats[...], axis=0)
    trust, decay = [], []
    for l in range(layers):
        wsq = jnp.sum(jnp.where(lane1 == l, total, 0.0), axis=(0, 1), keepdims=True)
        gsq = jnp.sum(jnp.where(lane1 == layers + l, total, 0.0), axis=(0, 1), keepdims=True)
        wnorm = jnp.sqrt(jnp.broadcast_to(wsq, (8, 128)))
        gnorm = jnp.sqrt(jnp.broadcast_to(gsq, (8, 128)))
        skipped = skip_ref[l].astype(jnp.float32)
        ratio = 0.02 * wnorm / (gnorm + 0.001 * wnorm + 1e-06)
        trust.append(skipped + (1.0 - skipped) * ratio)
        decay.append((1.0 - skipped) * 0.001)

    @pl.loop(0, span)
    def _(t):
        pos = place + t * TILE
        trust_pos = jnp.zeros((8, 128), jnp.float32)
        decay_pos = jnp.zeros((8, 128), jnp.float32)
        for l in range(layers):
            inside = (pos >= low[l]) & (pos < high[l])
            trust_pos = jnp.where(inside, trust[l], trust_pos)
            decay_pos = jnp.where(inside, decay[l], decay_pos)
        m = mv[t, 0]
        nv = 0.9 * mv[t, 1] + 8.0 * trust_pos * (grad_buf[t] + decay_pos * m)
        nm = m - nv
        nvw[t] = nv
        nmw[t] = nm
        ags[d, t] = nm.astype(jnp.bfloat16)

    def copy4(block, slot, dst):
        return pltpu.make_async_remote_copy(
            src_ref=ags.at[block],
            dst_ref=ags.at[block],
            send_sem=send4.at[slot],
            recv_sem=got4.at[block],
            device_id=dev(dst),
            device_id_type=MESH,
        )

    n_same = plane // 2
    me_same = a * n_spa + s
    partner = z * plane + a * (2 * n_spa) + (1 - c) * n_spa + s

    def same(index, core):
        return (index // n_spa) * (2 * n_spa) + core * n_spa + index % n_spa

    def put(block):
        return pltpu.make_async_copy(
            ags.at[block, pl.ds(0, step)], out_ref.at[pl.ds(block * step, step)], out_sem.at[block]
        )

    def to_plane(zz):
        block = zz * plane + p

        @pl.loop(1, n_same)
        def _(q):
            peer = (me_same + q) % n_same
            copy4(block, n_out + zz * n_same + peer, z * plane + same(peer, c)).start()

    def to_partner(zz, index):
        block = zz * plane + same(index, c)
        copy4(block, n_out + n_out * n_same + zz * n_same + index, partner).start()
        put(block).start()

    @pl.loop(1, n_out)
    def _(k):
        zz = (z + k) % n_out
        copy4(d, zz, zz * plane + p).start()

    to_plane(z)
    to_partner(z, me_same)

    back_l = 128 - shift_l
    for ref, src in ((nm_ref, nmw), (nv_ref, nvw)):
        x = src[...].reshape(rows, 128)
        x = pltpu.roll(x, (rows - shift_r) % rows, 0)
        x = pltpu.roll(x, back_l % 128, 1)
        ref[...] = jnp.where(lane < back_l, x, pltpu.roll(x, rows - 1, 0))

    @pl.loop(1, n_out)
    def _(k):
        zz = (z + k) % n_out
        copy4(zz * plane + p, zz, d).wait_recv()
        to_plane(zz)
        to_partner(zz, me_same)

    @pl.loop(0, n_out)
    def _(k):
        zz = (z + k) % n_out

        @pl.loop(1, n_same)
        def _(q):
            peer = (me_same + q) % n_same
            copy4(zz * plane + same(peer, c), 0, d).wait_recv()
            to_partner(zz, peer)

    @pl.loop(0, n_out)
    def _(k):
        zz = (z + k) % n_out

        @pl.loop(0, n_same)
        def _(q):
            peer = (me_same + q) % n_same
            block = zz * plane + same(peer, 1 - c)
            copy4(block, 0, d).wait_recv()
            put(block).start()

    tail = pltpu.make_async_copy(
        ags.at[n - 1, pl.ds(step, span - step)],
        out_ref.at[pl.ds(n * step, span - step)],
        out_sem.at[n],
    )
    tail.start()

    @pl.loop(1, n_out)
    def _(k):
        zz = (z + k) % n_out
        copy2(zz, z).wait_send()
        copy4(d, zz, zz * plane + p).wait_send()

    @pl.loop(0, n_out)
    def _(zz):
        @pl.loop(1, plane)
        def _(q):
            copy1(zz, p, (p + q) % plane).wait_send()

        @pl.loop(1, n_same)
        def _(q):
            peer = (me_same + q) % n_same
            copy4(zz * plane + p, n_out + zz * n_same + peer, z * plane + same(peer, c)).wait_send()

        @pl.loop(0, n_same)
        def _(index):
            slot = n_out + n_out * n_same + zz * n_same + index
            copy4(zz * plane + same(index, c), slot, partner).wait_send()

    @pl.loop(1, n)
    def _(q):
        copy3(d, (d + q) % n).wait_send()

    @pl.loop(0, n)
    def _(block):
        put(block).wait()

    tail.wait()


def windowed(n_rep, n_spa, grads, master, velocity, layer_offsets, layer_sizes, lars_skip):
    shard = master.shape[0]
    params = grads.shape[2]
    layers = layer_offsets.shape[0]
    n_in = math.isqrt(n_rep)
    n_out, n_a = n_rep // n_in, n_in // 2
    n = n_rep * n_spa
    plane = n_in * n_spa
    step = shard // TILE
    span = params // TILE - (n - 1) * step
    chunk = (plane - 1) * step + span
    tiles = params // TILE
    rows = span * 8
    pad = span * TILE - shard
    plan = (n_out, n_a, n_spa, shard, step, span, layers)
    vmem = pl.BlockSpec(memory_space=pltpu.VMEM)
    smem = pl.BlockSpec(memory_space=pltpu.SMEM)
    anywhere = pl.BlockSpec(memory_space=pl.ANY)
    f32, bf16 = jnp.float32, jnp.bfloat16
    dma = pltpu.SemaphoreType.DMA
    n_same = plane // 2
    weights, nm, nv = pl.pallas_call(
        functools.partial(kernel, plan),
        out_shape=(
            jax.ShapeDtypeStruct((tiles, 8, 128), bf16),
            jax.ShapeDtypeStruct((rows, 128), f32),
            jax.ShapeDtypeStruct((rows, 128), f32),
        ),
        in_specs=[anywhere, vmem, vmem, smem, smem, smem],
        out_specs=(anywhere, vmem, vmem),
        scratch_shapes=[
            pltpu.VMEM((n_out, 1, chunk * TILE), bf16),
            pltpu.VMEM((n_out, chunk, 8, 128), bf16),
            pltpu.VMEM((n_out, plane, span, 8, 128), bf16),
            pltpu.VMEM((n_out, span, 8, 128), f32),
            pltpu.VMEM((n_out, span, 8, 128), f32),
            pltpu.VMEM((span, 2, 8, 128), f32),
            pltpu.VMEM((2, 8, 128), f32),
            pltpu.VMEM((span, 8, 128), f32),
            pltpu.VMEM((1, 128), f32),
            pltpu.VMEM((n, 1, 128), f32),
            pltpu.VMEM((n, span, 8, 128), bf16),
            pltpu.VMEM((span, 8, 128), f32),
            pltpu.VMEM((span, 8, 128), f32),
            dma((n_out,)),
            dma((n_out, plane)),
            dma((n_out, plane)),
            dma((n_out,)),
            dma((n_out,)),
            dma((2,)),
            dma((n,)),
            dma((n,)),
            dma((n_out + 2 * n_out * n_same,)),
            dma((n,)),
            dma((n + 1,)),
        ],
        compiler_params=pltpu.CompilerParams(collective_id=0, has_side_effects=True),
    )(
        grads,
        jnp.pad(master, (0, pad)).reshape(rows, 128),
        jnp.pad(velocity, (0, pad)).reshape(rows, 128),
        layer_offsets,
        layer_sizes,
        lars_skip,
    )
    return weights.reshape(params), nm.reshape(-1)[:shard], nv.reshape(-1)[:shard]


def tiled(n_rep, n_spa, params):
    n = n_rep * n_spa
    shard = params // n
    n_in = math.isqrt(n_rep)
    rest = shard % TILE
    return (
        n_in * n_in == n_rep
        and n_in % 2 == 0
        and params % TILE == 0
        and shard >= TILE
        and 0 < n * rest <= TILE
    )


def step_fn(n_rep, n_spa, grads, *rest):
    if tiled(n_rep, n_spa, grads.shape[2]):
        return windowed(n_rep, n_spa, grads, *rest)
    return shards(grads, *rest)


def shards(grads, master, velocity, layer_offsets, layer_sizes, lars_skip):
    n_rep = lax.axis_size("replica")
    n_spa = lax.axis_size("spatial")
    shard = master.shape[0]
    position = lax.axis_index(("replica", "spatial")) * shard + jnp.arange(shard, dtype=jnp.int32)
    inside = (position[None, :] >= layer_offsets[:, None]) & (
        position[None, :] < (layer_offsets + layer_sizes)[:, None]
    )
    onehot = inside.astype(jnp.float32)
    received = lax.all_to_all(
        grads[0, 0].reshape(n_rep, n_spa * shard),
        "replica",
        split_axis=0,
        concat_axis=0,
        tiled=True,
    )
    first = jnp.sum(received.astype(jnp.float32), axis=0)
    summed = lax.psum_scatter(
        first.reshape(n_spa, shard), "spatial", scatter_dimension=0, tiled=True
    )
    grad = summed.reshape(shard) / (n_rep * n_spa)
    gsq_local = jnp.dot(onehot, grad * grad, precision=lax.Precision.HIGHEST)
    wsq_local = jnp.dot(onehot, master * master, precision=lax.Precision.HIGHEST)
    wsq, gsq = lax.psum((wsq_local, gsq_local), ("replica", "spatial"))
    wnorm = jnp.sqrt(wsq)
    gnorm = jnp.sqrt(gsq)
    skipped = lars_skip.astype(jnp.float32)
    ratio = 0.02 * wnorm / (gnorm + 0.001 * wnorm + 1e-06)
    trust = skipped + (1.0 - skipped) * ratio
    decay = (1.0 - skipped) * 0.001
    trust_pos = jnp.dot(trust, onehot, precision=lax.Precision.HIGHEST)
    decay_pos = jnp.dot(decay, onehot, precision=lax.Precision.HIGHEST)
    new_velocity = 0.9 * velocity + 8.0 * trust_pos * (grad + decay_pos * master)
    new_master = master - new_velocity
    new_weights = lax.all_gather(
        new_master.astype(jnp.bfloat16), ("replica", "spatial"), axis=0, tiled=True
    )
    return (new_weights, new_master, new_velocity)


def solution(mesh):
    return jax.shard_map(
        functools.partial(step_fn, mesh.shape["replica"], mesh.shape["spatial"]),
        mesh=mesh,
        in_specs=(
            P("replica", "spatial", None),
            P(("replica", "spatial")),
            P(("replica", "spatial")),
            P(),
            P(),
            P(),
        ),
        out_specs=(P(), P(("replica", "spatial")), P(("replica", "spatial"))),
        check_vma=False,
    )
```

```python
import functools
import math

import jax
import jax.numpy as jnp
from jax import lax
from jax.experimental import pallas as pl
from jax.experimental.pallas import tpu as pltpu
from jax.sharding import PartitionSpec as P

MESH = pl.DeviceIdType.MESH
TILE = 1024


def kernel(
    plan,
    grads_ref,
    m_ref,
    v_ref,
    offsets_ref,
    sizes_ref,
    skip_ref,
    ags,
    nmw,
    nvw,
    m_in,
    v_in,
    gin,
    packed,
    recv1,
    part,
    recv2,
    mv,
    halo,
    grad_buf,
    wrow,
    stats,
    in_sem,
    mv_sem,
    send1,
    got1,
    send2,
    got2,
    halo_sem,
    send3,
    got3,
    send4,
    got4,
):
    n_out, n_a, n_spa, shard, step, span, layers = plan
    plane = n_a * 2 * n_spa
    n = n_out * plane
    chunk = (plane - 1) * step + span
    rows = span * 8
    r = lax.axis_index("replica")
    s = lax.axis_index("spatial")
    d = r * n_spa + s
    z = d // plane
    p = d % plane
    a = p // (2 * n_spa)
    c = (p // n_spa) % 2
    base = d * (step * TILE)
    off = d * (shard - step * TILE)

    def dev(flat):
        return (flat // n_spa, flat % n_spa)

    barrier = pltpu.get_barrier_semaphore()

    @pl.loop(1, n)
    def _(q):
        pl.semaphore_signal(barrier, inc=1, device_id=dev((d + q) % n), device_id_type=MESH)

    def load(zt):
        start = pl.multiple_of(zt * (plane * step * TILE), TILE)
        return pltpu.make_async_copy(
            grads_ref.at[0, :, pl.ds(start, chunk * TILE)], gin.at[zt], in_sem.at[zt]
        )

    for k in range(1, n_out + 1):
        load((z + k) % n_out).start()
    mv_loads = [
        pltpu.make_async_copy(ref, buf, mv_sem.at[j])
        for j, (ref, buf) in enumerate(((m_ref, m_in), (v_ref, v_in)))
    ]
    for copy in mv_loads:
        copy.start()

    group = max(g for g in range(1, 33) if chunk % g == 0)

    def pack(zt):
        load(zt).wait()

        @pl.loop(0, chunk // group)
        def _(i):
            at = pl.multiple_of(i * (group * TILE), group * TILE)
            v = gin[zt, :, pl.ds(at, group * TILE)].astype(jnp.float32)
            packed[zt, pl.ds(i * group, group)] = v.reshape(group, 8, 128).astype(jnp.bfloat16)

    def copy1(zt, src, dst):
        return pltpu.make_async_remote_copy(
            src_ref=packed.at[zt, pl.ds(dst * step, span)],
            dst_ref=recv1.at[zt, src],
            send_sem=send1.at[zt, dst],
            recv_sem=got1.at[zt, src],
            device_id=dev(z * plane + dst),
            device_id_type=MESH,
        )

    for k in range(1, n_out + 1):
        zt = (z + k) % n_out
        pack(zt)
        if k == 1:
            pl.semaphore_wait(barrier, n - 1)

        @pl.loop(1, plane)
        def _(q):
            copy1(zt, p, (p + q) % plane).start()

    lane = lax.broadcasted_iota(jnp.int32, (rows, 128), 1)
    shift_l = off % 128
    shift_r = off // 128
    whole = step * TILE
    for j, ref in enumerate((m_in, v_in)):
        mv_loads[j].wait()
        edge = jnp.pad(ref[pl.ds(whole, shard - whole)], (0, 128 - (shard - whole)))
        edge = jnp.broadcast_to(edge.reshape(1, 128), (8, 128))
        x = jnp.concatenate([ref[pl.ds(0, whole)].reshape(step * 8, 128), edge], 0)
        x = pltpu.roll(x, shift_l, 1)
        x = jnp.where(lane < shift_l, pltpu.roll(x, 1, 0), x)
        x = pltpu.roll(x, shift_r, 0)
        mv[:, j] = x.reshape(span, 8, 128)
    halo_copy = pltpu.make_async_remote_copy(
        src_ref=mv.at[span - 1],
        dst_ref=halo,
        send_sem=halo_sem.at[0],
        recv_sem=halo_sem.at[1],
        device_id=dev((d + 1) % n),
        device_id_type=MESH,
    )
    halo_copy.start()

    place = lax.broadcasted_iota(jnp.int32, (8, 128), 0) * 128 + lax.broadcasted_iota(
        jnp.int32, (8, 128), 1
    )
    low = [offsets_ref[l] - base for l in range(layers)]
    high = [offsets_ref[l] + sizes_ref[l] - base for l in range(layers)]
    own_low = [jnp.maximum(x, off) for x in low]
    own_high = [jnp.minimum(x, off + shard) for x in high]
    lane1 = lax.broadcasted_iota(jnp.int32, (1, 128), 1)

    def squares(value, first):
        def add(t, accs):
            pos = place + t * TILE
            x = value(t)
            x = x * x
            return tuple(
                acc + jnp.where((pos >= lo) & (pos < hi), x, 0.0)
                for acc, lo, hi in zip(accs, own_low, own_high)
            )

        accs = lax.fori_loop(
            0, span, add, tuple(jnp.zeros((8, 128), jnp.float32) for _ in range(layers))
        )
        row = jnp.zeros((1, 128), jnp.float32)
        for l, acc in enumerate(accs):
            row = jnp.where(lane1 == first + l, jnp.sum(acc, axis=(0, 1), keepdims=True), row)
        return row

    wrow[...] = squares(lambda t: mv[t, 0], 0)

    def copy2(zt, src):
        return pltpu.make_async_remote_copy(
            src_ref=part.at[zt],
            dst_ref=recv2.at[src],
            send_sem=send2.at[zt],
            recv_sem=got2.at[src],
            device_id=dev(zt * plane + p),
            device_id_type=MESH,
        )

    for k in range(1, n_out + 1):
        zt = (z + k) % n_out

        @pl.loop(1, plane)
        def _(q):
            copy1(zt, (p + q) % plane, p).wait_recv()

        @pl.loop(0, span)
        def _(t):
            acc = packed[zt, p * step + t].astype(jnp.float32)
            for q in range(1, plane):
                acc = acc + recv1[zt, (p + q) % plane, t].astype(jnp.float32)
            part[zt, t] = acc

        if k < n_out:
            copy2(zt, z).start()

    halo_copy.wait()
    for j in range(2):
        mv[0, j] = jnp.where(place < off, halo[j], mv[0, j])

    @pl.loop(1, n_out)
    def _(k):
        copy2(z, (z + k) % n_out).wait_recv()

    @pl.loop(0, span)
    def _(t):
        acc = part[z, t]
        for k in range(1, n_out):
            acc = acc + recv2[(z + k) % n_out, t]
        grad_buf[t] = acc / n

    stats[d] = squares(lambda t: grad_buf[t], layers) + wrow[...]

    def copy3(src, dst):
        return pltpu.make_async_remote_copy(
            src_ref=stats.at[src],
            dst_ref=stats.at[src],
            send_sem=send3.at[dst],
            recv_sem=got3.at[src],
            device_id=dev(dst),
            device_id_type=MESH,
        )

    @pl.loop(1, n)
    def _(q):
        copy3(d, (d + q) % n).start()

    @pl.loop(1, n)
    def _(q):
        copy3((d + q) % n, d).wait_recv()

    total = jnp.sum(stats[...], axis=0)
    trust, decay = [], []
    for l in range(layers):
        wsq = jnp.sum(jnp.where(lane1 == l, total, 0.0), axis=(0, 1), keepdims=True)
        gsq = jnp.sum(jnp.where(lane1 == layers + l, total, 0.0), axis=(0, 1), keepdims=True)
        wnorm = jnp.sqrt(jnp.broadcast_to(wsq, (8, 128)))
        gnorm = jnp.sqrt(jnp.broadcast_to(gsq, (8, 128)))
        skipped = skip_ref[l].astype(jnp.float32)
        ratio = 0.02 * wnorm / (gnorm + 0.001 * wnorm + 1e-06)
        trust.append(skipped + (1.0 - skipped) * ratio)
        decay.append((1.0 - skipped) * 0.001)

    @pl.loop(0, span)
    def _(t):
        pos = place + t * TILE
        trust_pos = jnp.zeros((8, 128), jnp.float32)
        decay_pos = jnp.zeros((8, 128), jnp.float32)
        for l in range(layers):
            inside = (pos >= low[l]) & (pos < high[l])
            trust_pos = jnp.where(inside, trust[l], trust_pos)
            decay_pos = jnp.where(inside, decay[l], decay_pos)
        m = mv[t, 0]
        nv = 0.9 * mv[t, 1] + 8.0 * trust_pos * (grad_buf[t] + decay_pos * m)
        nm = m - nv
        nvw[t] = nv
        nmw[t] = nm
        ags[d, t] = nm.astype(jnp.bfloat16)

    def copy4(block, slot, dst):
        return pltpu.make_async_remote_copy(
            src_ref=ags.at[block],
            dst_ref=ags.at[block],
            send_sem=send4.at[slot],
            recv_sem=got4.at[block],
            device_id=dev(dst),
            device_id_type=MESH,
        )

    n_same = plane // 2
    me_same = a * n_spa + s
    partner = z * plane + a * (2 * n_spa) + (1 - c) * n_spa + s

    def same(index, core):
        return (index // n_spa) * (2 * n_spa) + core * n_spa + index % n_spa

    def to_plane(zz):
        block = zz * plane + p

        @pl.loop(1, n_same)
        def _(q):
            peer = (me_same + q) % n_same
            copy4(block, n_out + zz * n_same + peer, z * plane + same(peer, c)).start()

    def to_partner(zz, index):
        block = zz * plane + same(index, c)
        copy4(block, n_out + n_out * n_same + zz * n_same + index, partner).start()

    @pl.loop(1, n_out)
    def _(k):
        zz = (z + k) % n_out
        copy4(d, zz, zz * plane + p).start()

    to_plane(z)
    to_partner(z, me_same)

    @pl.loop(1, n_out)
    def _(k):
        zz = (z + k) % n_out
        copy4(zz * plane + p, zz, d).wait_recv()
        to_plane(zz)
        to_partner(zz, me_same)

    @pl.loop(0, n_out)
    def _(k):
        zz = (z + k) % n_out

        @pl.loop(1, n_same)
        def _(q):
            peer = (me_same + q) % n_same
            copy4(zz * plane + same(peer, c), 0, d).wait_recv()
            to_partner(zz, peer)

    @pl.loop(0, n_out)
    def _(k):
        zz = (z + k) % n_out

        @pl.loop(0, n_same)
        def _(q):
            peer = (me_same + q) % n_same
            block = zz * plane + same(peer, 1 - c)
            copy4(block, 0, d).wait_recv()

    @pl.loop(1, n_out)
    def _(k):
        zz = (z + k) % n_out
        copy2(zz, z).wait_send()
        copy4(d, zz, zz * plane + p).wait_send()

    @pl.loop(0, n_out)
    def _(zz):
        @pl.loop(1, plane)
        def _(q):
            copy1(zz, p, (p + q) % plane).wait_send()

        @pl.loop(1, n_same)
        def _(q):
            peer = (me_same + q) % n_same
            copy4(zz * plane + p, n_out + zz * n_same + peer, z * plane + same(peer, c)).wait_send()

        @pl.loop(0, n_same)
        def _(index):
            slot = n_out + n_out * n_same + zz * n_same + index
            copy4(zz * plane + same(index, c), slot, partner).wait_send()

    @pl.loop(1, n)
    def _(q):
        copy3(d, (d + q) % n).wait_send()


def finish(plan, ags, nmw, nvw, out_ref, nm_ref, nv_ref, nm_out, nv_out, out_sem, own_sem):
    n, n_spa, shard, step, span = plan
    rows = span * 8
    whole = step * TILE
    copies = [
        pltpu.make_async_copy(
            ags.at[b, pl.ds(0, step)], out_ref.at[pl.ds(b * step, step)], out_sem.at[b]
        )
        for b in range(n)
    ]
    copies.append(
        pltpu.make_async_copy(
            ags.at[n - 1, pl.ds(step, span - step)],
            out_ref.at[pl.ds(n * step, span - step)],
            out_sem.at[n],
        )
    )
    for copy in copies:
        copy.start()
    d = lax.axis_index("replica") * n_spa + lax.axis_index("spatial")
    off = d * (shard - whole)
    shift_l = off % 128
    shift_r = off // 128
    back_l = 128 - shift_l
    lane = lax.broadcasted_iota(jnp.int32, (rows, 128), 1)
    for j, (src, buf, ref) in enumerate(((nmw, nm_out, nm_ref), (nvw, nv_out, nv_ref))):
        x = src[...].reshape(rows, 128)
        x = pltpu.roll(x, (rows - shift_r) % rows, 0)
        x = pltpu.roll(x, back_l % 128, 1)
        x = jnp.where(lane < back_l, x, pltpu.roll(x, rows - 1, 0))
        buf[pl.ds(0, whole)] = x[: step * 8].reshape(whole)
        buf[pl.ds(whole, shard - whole)] = x[step * 8, : shard - whole].reshape(shard - whole)
        copy = pltpu.make_async_copy(buf, ref, own_sem.at[j])
        copy.start()
        copies.append(copy)
    for copy in copies:
        copy.wait()


def windowed(n_rep, n_spa, grads, master, velocity, layer_offsets, layer_sizes, lars_skip):
    shard = master.shape[0]
    params = grads.shape[2]
    layers = layer_offsets.shape[0]
    n_in = math.isqrt(n_rep)
    n_out, n_a = n_rep // n_in, n_in // 2
    n = n_rep * n_spa
    plane = n_in * n_spa
    step = shard // TILE
    span = params // TILE - (n - 1) * step
    chunk = (plane - 1) * step + span
    tiles = params // TILE
    plan = (n_out, n_a, n_spa, shard, step, span, layers)
    vmem = pl.BlockSpec(memory_space=pltpu.VMEM)
    smem = pl.BlockSpec(memory_space=pltpu.SMEM)
    anywhere = pl.BlockSpec(memory_space=pltpu.HBM)
    f32, bf16 = jnp.float32, jnp.bfloat16
    dma = pltpu.SemaphoreType.DMA
    n_same = plane // 2
    ags, nmw, nvw = pl.pallas_call(
        functools.partial(kernel, plan),
        out_shape=(
            pltpu.VMEM((n, span, 8, 128), bf16),
            pltpu.VMEM((span, 8, 128), f32),
            pltpu.VMEM((span, 8, 128), f32),
        ),
        in_specs=[anywhere, anywhere, anywhere, smem, smem, smem],
        out_specs=(vmem, vmem, vmem),
        scratch_shapes=[
            pltpu.VMEM((shard,), f32),
            pltpu.VMEM((shard,), f32),
            pltpu.VMEM((n_out, 1, chunk * TILE), bf16),
            pltpu.VMEM((n_out, chunk, 8, 128), bf16),
            pltpu.VMEM((n_out, plane, span, 8, 128), bf16),
            pltpu.VMEM((n_out, span, 8, 128), f32),
            pltpu.VMEM((n_out, span, 8, 128), f32),
            pltpu.VMEM((span, 2, 8, 128), f32),
            pltpu.VMEM((2, 8, 128), f32),
            pltpu.VMEM((span, 8, 128), f32),
            pltpu.VMEM((1, 128), f32),
            pltpu.VMEM((n, 1, 128), f32),
            dma((n_out,)),
            dma((2,)),
            dma((n_out, plane)),
            dma((n_out, plane)),
            dma((n_out,)),
            dma((n_out,)),
            dma((2,)),
            dma((n,)),
            dma((n,)),
            dma((n_out + 2 * n_out * n_same,)),
            dma((n,)),
        ],
        compiler_params=pltpu.CompilerParams(
            collective_id=0, has_side_effects=True, vmem_limit_bytes=61 * 2**20
        ),
    )(grads, master, velocity, layer_offsets, layer_sizes, lars_skip)
    weights, nm, nv = pl.pallas_call(
        functools.partial(finish, (n, n_spa, shard, step, span)),
        out_shape=(
            jax.ShapeDtypeStruct((tiles, 8, 128), bf16),
            jax.ShapeDtypeStruct((shard,), f32),
            jax.ShapeDtypeStruct((shard,), f32),
        ),
        in_specs=[vmem, vmem, vmem],
        out_specs=(anywhere, anywhere, anywhere),
        scratch_shapes=[
            pltpu.VMEM((shard,), f32),
            pltpu.VMEM((shard,), f32),
            dma((n + 1,)),
            dma((2,)),
        ],
        compiler_params=pltpu.CompilerParams(vmem_limit_bytes=16 * 2**20),
    )(ags, nmw, nvw)
    return weights.reshape(params), nm, nv


def tiled(n_rep, n_spa, params):
    n = n_rep * n_spa
    shard = params // n
    n_in = math.isqrt(n_rep)
    rest = shard % TILE
    return (
        n_in * n_in == n_rep
        and n_in % 2 == 0
        and params % TILE == 0
        and shard >= TILE
        and 0 < n * rest <= TILE
        and rest <= 128
    )


def step_fn(n_rep, n_spa, grads, *rest):
    if tiled(n_rep, n_spa, grads.shape[2]):
        return windowed(n_rep, n_spa, grads, *rest)
    return shards(grads, *rest)


def shards(grads, master, velocity, layer_offsets, layer_sizes, lars_skip):
    n_rep = lax.axis_size("replica")
    n_spa = lax.axis_size("spatial")
    shard = master.shape[0]
    position = lax.axis_index(("replica", "spatial")) * shard + jnp.arange(shard, dtype=jnp.int32)
    inside = (position[None, :] >= layer_offsets[:, None]) & (
        position[None, :] < (layer_offsets + layer_sizes)[:, None]
    )
    onehot = inside.astype(jnp.float32)
    received = lax.all_to_all(
        grads[0, 0].reshape(n_rep, n_spa * shard),
        "replica",
        split_axis=0,
        concat_axis=0,
        tiled=True,
    )
    first = jnp.sum(received.astype(jnp.float32), axis=0)
    summed = lax.psum_scatter(
        first.reshape(n_spa, shard), "spatial", scatter_dimension=0, tiled=True
    )
    grad = summed.reshape(shard) / (n_rep * n_spa)
    gsq_local = jnp.dot(onehot, grad * grad, precision=lax.Precision.HIGHEST)
    wsq_local = jnp.dot(onehot, master * master, precision=lax.Precision.HIGHEST)
    wsq, gsq = lax.psum((wsq_local, gsq_local), ("replica", "spatial"))
    wnorm = jnp.sqrt(wsq)
    gnorm = jnp.sqrt(gsq)
    skipped = lars_skip.astype(jnp.float32)
    ratio = 0.02 * wnorm / (gnorm + 0.001 * wnorm + 1e-06)
    trust = skipped + (1.0 - skipped) * ratio
    decay = (1.0 - skipped) * 0.001
    trust_pos = jnp.dot(trust, onehot, precision=lax.Precision.HIGHEST)
    decay_pos = jnp.dot(decay, onehot, precision=lax.Precision.HIGHEST)
    new_velocity = 0.9 * velocity + 8.0 * trust_pos * (grad + decay_pos * master)
    new_master = master - new_velocity
    new_weights = lax.all_gather(
        new_master.astype(jnp.bfloat16), ("replica", "spatial"), axis=0, tiled=True
    )
    return (new_weights, new_master, new_velocity)


def solution(mesh):
    return jax.shard_map(
        functools.partial(step_fn, mesh.shape["replica"], mesh.shape["spatial"]),
        mesh=mesh,
        in_specs=(
            P("replica", "spatial", None),
            P(("replica", "spatial")),
            P(("replica", "spatial")),
            P(),
            P(),
            P(),
        ),
        out_specs=(P(), P(("replica", "spatial")), P(("replica", "spatial"))),
        check_vma=False,
    )
```

```python
import functools
import math

import jax
import jax.numpy as jnp
from jax import lax
from jax.experimental import pallas as pl
from jax.experimental.pallas import tpu as pltpu
from jax.sharding import PartitionSpec as P

MESH = pl.DeviceIdType.MESH
TILE = 1024


def kernel(
    plan,
    grads_ref,
    m_ref,
    v_ref,
    offsets_ref,
    sizes_ref,
    skip_ref,
    ags,
    nmw,
    nvw,
    m_in,
    v_in,
    gin,
    packed,
    recv1,
    part,
    recv2,
    mv,
    halo,
    grad_buf,
    wrow,
    stats,
    in_sem,
    mv_sem,
    send1,
    got1,
    send2,
    got2,
    halo_sem,
    send3,
    got3,
    send4,
    got4,
):
    n_out, n_a, n_spa, shard, step, span, layers = plan
    plane = n_a * 2 * n_spa
    n = n_out * plane
    chunk = (plane - 1) * step + span
    rows = span * 8
    r = lax.axis_index("replica")
    s = lax.axis_index("spatial")
    d = r * n_spa + s
    z = d // plane
    p = d % plane
    a = p // (2 * n_spa)
    c = (p // n_spa) % 2
    base = d * (step * TILE)
    off = d * (shard - step * TILE)

    def dev(flat):
        return (flat // n_spa, flat % n_spa)

    barrier = pltpu.get_barrier_semaphore()

    def load(zt):
        start = pl.multiple_of(zt * (plane * step * TILE), TILE)
        return pltpu.make_async_copy(
            grads_ref.at[0, :, pl.ds(start, chunk * TILE)], gin.at[zt], in_sem.at[zt]
        )

    for k in range(1, n_out + 1):
        load((z + k) % n_out).start()
    mv_loads = [
        pltpu.make_async_copy(ref, buf, mv_sem.at[j])
        for j, (ref, buf) in enumerate(((m_ref, m_in), (v_ref, v_in)))
    ]
    for copy in mv_loads:
        copy.start()

    @pl.loop(1, n, unroll=True)
    def _(q):
        pl.semaphore_signal(barrier, inc=1, device_id=dev((d + q) % n), device_id_type=MESH)

    group = max(g for g in range(1, 33) if chunk % g == 0)

    def pack(zt):
        load(zt).wait()

        @pl.loop(0, chunk // group)
        def _(i):
            at = pl.multiple_of(i * (group * TILE), group * TILE)
            v = gin[zt, :, pl.ds(at, group * TILE)].astype(jnp.float32)
            packed[zt, pl.ds(i * group, group)] = v.reshape(group, 8, 128).astype(jnp.bfloat16)

    def copy1(zt, src, dst):
        return pltpu.make_async_remote_copy(
            src_ref=packed.at[zt, pl.ds(dst * step, span)],
            dst_ref=recv1.at[zt, src],
            send_sem=send1,
            recv_sem=got1.at[zt, src],
            device_id=dev(z * plane + dst),
            device_id_type=MESH,
        )

    for k in range(1, n_out + 1):
        zt = (z + k) % n_out
        pack(zt)
        if k == 1:
            pl.semaphore_wait(barrier, n - 1)

        @pl.loop(1, plane, unroll=True)
        def _(q):
            copy1(zt, p, (p + q) % plane).start()

    lane = lax.broadcasted_iota(jnp.int32, (rows, 128), 1)
    shift_l = off % 128
    shift_r = off // 128
    whole = step * TILE
    for j, ref in enumerate((m_in, v_in)):
        mv_loads[j].wait()
        edge = jnp.pad(ref[pl.ds(whole, shard - whole)], (0, 128 - (shard - whole)))
        edge = jnp.broadcast_to(edge.reshape(1, 128), (8, 128))
        x = jnp.concatenate([ref[pl.ds(0, whole)].reshape(step * 8, 128), edge], 0)
        x = pltpu.roll(x, shift_l, 1)
        x = jnp.where(lane < shift_l, pltpu.roll(x, 1, 0), x)
        x = pltpu.roll(x, shift_r, 0)
        mv[:, j] = x.reshape(span, 8, 128)
    halo_copy = pltpu.make_async_remote_copy(
        src_ref=mv.at[span - 1],
        dst_ref=halo,
        send_sem=halo_sem.at[0],
        recv_sem=halo_sem.at[1],
        device_id=dev((d + 1) % n),
        device_id_type=MESH,
    )
    halo_copy.start()

    place = lax.broadcasted_iota(jnp.int32, (8, 128), 0) * 128 + lax.broadcasted_iota(
        jnp.int32, (8, 128), 1
    )
    low = [offsets_ref[l] - base for l in range(layers)]
    high = [offsets_ref[l] + sizes_ref[l] - base for l in range(layers)]
    own_low = [jnp.maximum(x, off) for x in low]
    own_high = [jnp.minimum(x, off + shard) for x in high]
    lane1 = lax.broadcasted_iota(jnp.int32, (1, 128), 1)

    def squares(value, first):
        def add(t, accs):
            pos = place + t * TILE
            x = value(t)
            x = x * x
            return tuple(
                acc + jnp.where((pos >= lo) & (pos < hi), x, 0.0)
                for acc, lo, hi in zip(accs, own_low, own_high)
            )

        accs = lax.fori_loop(
            0, span, add, tuple(jnp.zeros((8, 128), jnp.float32) for _ in range(layers))
        )
        row = jnp.zeros((1, 128), jnp.float32)
        for l, acc in enumerate(accs):
            row = jnp.where(lane1 == first + l, jnp.sum(acc, axis=(0, 1), keepdims=True), row)
        return row

    wrow[...] = squares(lambda t: mv[t, 0], 0)

    def copy2(zt, src):
        return pltpu.make_async_remote_copy(
            src_ref=part.at[zt],
            dst_ref=recv2.at[src],
            send_sem=send2,
            recv_sem=got2.at[src],
            device_id=dev(zt * plane + p),
            device_id_type=MESH,
        )

    for k in range(1, n_out + 1):
        zt = (z + k) % n_out

        @pl.loop(1, plane)
        def _(q):
            copy1(zt, (p + q) % plane, p).wait_recv()

        @pl.loop(0, span)
        def _(t):
            acc = packed[zt, p * step + t].astype(jnp.float32)
            for q in range(1, plane):
                acc = acc + recv1[zt, (p + q) % plane, t].astype(jnp.float32)
            part[zt, t] = acc

        if k < n_out:
            copy2(zt, z).start()

    halo_copy.wait()
    for j in range(2):
        mv[0, j] = jnp.where(place < off, halo[j], mv[0, j])

    @pl.loop(1, n_out)
    def _(k):
        copy2(z, (z + k) % n_out).wait_recv()

    @pl.loop(0, span)
    def _(t):
        acc = part[z, t]
        for k in range(1, n_out):
            acc = acc + recv2[(z + k) % n_out, t]
        grad_buf[t] = acc / n

    stats[d] = squares(lambda t: grad_buf[t], layers) + wrow[...]

    def copy3(src, dst):
        return pltpu.make_async_remote_copy(
            src_ref=stats.at[src],
            dst_ref=stats.at[src],
            send_sem=send3,
            recv_sem=got3.at[src],
            device_id=dev(dst),
            device_id_type=MESH,
        )

    @pl.loop(1, n, unroll=True)
    def _(q):
        copy3(d, (d + q) % n).start()

    @pl.loop(1, n, unroll=True)
    def _(q):
        copy3((d + q) % n, d).wait_recv()

    total = jnp.sum(stats[...], axis=0)
    trust, decay = [], []
    for l in range(layers):
        wsq = jnp.sum(jnp.where(lane1 == l, total, 0.0), axis=(0, 1), keepdims=True)
        gsq = jnp.sum(jnp.where(lane1 == layers + l, total, 0.0), axis=(0, 1), keepdims=True)
        wnorm = jnp.sqrt(jnp.broadcast_to(wsq, (8, 128)))
        gnorm = jnp.sqrt(jnp.broadcast_to(gsq, (8, 128)))
        skipped = skip_ref[l].astype(jnp.float32)
        ratio = 0.02 * wnorm / (gnorm + 0.001 * wnorm + 1e-06)
        trust.append(skipped + (1.0 - skipped) * ratio)
        decay.append((1.0 - skipped) * 0.001)

    @pl.loop(0, span)
    def _(t):
        pos = place + t * TILE
        trust_pos = jnp.zeros((8, 128), jnp.float32)
        decay_pos = jnp.zeros((8, 128), jnp.float32)
        for l in range(layers):
            inside = (pos >= low[l]) & (pos < high[l])
            trust_pos = jnp.where(inside, trust[l], trust_pos)
            decay_pos = jnp.where(inside, decay[l], decay_pos)
        m = mv[t, 0]
        nv = 0.9 * mv[t, 1] + 8.0 * trust_pos * (grad_buf[t] + decay_pos * m)
        nm = m - nv
        nvw[t] = nv
        nmw[t] = nm
        ags[d, t] = nm.astype(jnp.bfloat16)

    def copy4(block, dst):
        return pltpu.make_async_remote_copy(
            src_ref=ags.at[block],
            dst_ref=ags.at[block],
            send_sem=send4,
            recv_sem=got4.at[block],
            device_id=dev(dst),
            device_id_type=MESH,
        )

    n_same = plane // 2
    me_same = a * n_spa + s
    partner = z * plane + a * (2 * n_spa) + (1 - c) * n_spa + s

    def same(index, core):
        return (index // n_spa) * (2 * n_spa) + core * n_spa + index % n_spa

    def to_plane(zz):
        block = zz * plane + p

        @pl.loop(1, n_same)
        def _(q):
            peer = (me_same + q) % n_same
            copy4(block, z * plane + same(peer, c)).start()

    def to_partner(zz, index):
        block = zz * plane + same(index, c)
        copy4(block, partner).start()

    @pl.loop(1, n_out)
    def _(k):
        zz = (z + k) % n_out
        copy4(d, zz * plane + p).start()

    to_plane(z)
    to_partner(z, me_same)

    @pl.loop(1, n_out)
    def _(k):
        zz = (z + k) % n_out
        copy4(zz * plane + p, d).wait_recv()
        to_plane(zz)
        to_partner(zz, me_same)

    @pl.loop(0, n_out)
    def _(k):
        zz = (z + k) % n_out

        @pl.loop(1, n_same)
        def _(q):
            peer = (me_same + q) % n_same
            copy4(zz * plane + same(peer, c), d).wait_recv()
            to_partner(zz, peer)

    @pl.loop(0, n_out)
    def _(k):
        zz = (z + k) % n_out

        @pl.loop(0, n_same)
        def _(q):
            peer = (me_same + q) % n_same
            block = zz * plane + same(peer, 1 - c)
            copy4(block, d).wait_recv()

    for ref, sem in (
        (recv1.at[:, pl.ds(0, plane - 1)], send1),
        (recv2.at[pl.ds(0, n_out - 1)], send2),
        (stats.at[pl.ds(0, n - 1)], send3),
        (ags.at[pl.ds(0, n - 1)], send4),
    ):
        pltpu.make_async_copy(ref, ref, sem).wait()


def finish(plan, ags, nmw, nvw, out_ref, nm_ref, nv_ref, nm_out, nv_out, out_sem, own_sem):
    n, n_spa, shard, step, span = plan
    rows = span * 8
    whole = step * TILE
    copies = [
        pltpu.make_async_copy(
            ags.at[b, pl.ds(0, step)], out_ref.at[pl.ds(b * step, step)], out_sem.at[b]
        )
        for b in range(n)
    ]
    copies.append(
        pltpu.make_async_copy(
            ags.at[n - 1, pl.ds(step, span - step)],
            out_ref.at[pl.ds(n * step, span - step)],
            out_sem.at[n],
        )
    )
    for copy in copies:
        copy.start()
    d = lax.axis_index("replica") * n_spa + lax.axis_index("spatial")
    off = d * (shard - whole)
    shift_l = off % 128
    shift_r = off // 128
    back_l = 128 - shift_l
    lane = lax.broadcasted_iota(jnp.int32, (rows, 128), 1)
    for j, (src, buf, ref) in enumerate(((nmw, nm_out, nm_ref), (nvw, nv_out, nv_ref))):
        x = src[...].reshape(rows, 128)
        x = pltpu.roll(x, (rows - shift_r) % rows, 0)
        x = pltpu.roll(x, back_l % 128, 1)
        x = jnp.where(lane < back_l, x, pltpu.roll(x, rows - 1, 0))
        buf[pl.ds(0, whole)] = x[: step * 8].reshape(whole)
        buf[pl.ds(whole, shard - whole)] = x[step * 8, : shard - whole].reshape(shard - whole)
        copy = pltpu.make_async_copy(buf, ref, own_sem.at[j])
        copy.start()
        copies.append(copy)
    for copy in copies:
        copy.wait()


def windowed(n_rep, n_spa, grads, master, velocity, layer_offsets, layer_sizes, lars_skip):
    shard = master.shape[0]
    params = grads.shape[2]
    layers = layer_offsets.shape[0]
    n_in = math.isqrt(n_rep)
    n_out, n_a = n_rep // n_in, n_in // 2
    n = n_rep * n_spa
    plane = n_in * n_spa
    step = shard // TILE
    span = params // TILE - (n - 1) * step
    chunk = (plane - 1) * step + span
    tiles = params // TILE
    plan = (n_out, n_a, n_spa, shard, step, span, layers)
    vmem = pl.BlockSpec(memory_space=pltpu.VMEM)
    smem = pl.BlockSpec(memory_space=pltpu.SMEM)
    anywhere = pl.BlockSpec(memory_space=pltpu.HBM)
    f32, bf16 = jnp.float32, jnp.bfloat16
    dma = pltpu.SemaphoreType.DMA
    ags, nmw, nvw = pl.pallas_call(
        functools.partial(kernel, plan),
        out_shape=(
            pltpu.VMEM((n, span, 8, 128), bf16),
            pltpu.VMEM((span, 8, 128), f32),
            pltpu.VMEM((span, 8, 128), f32),
        ),
        in_specs=[anywhere, anywhere, anywhere, smem, smem, smem],
        out_specs=(vmem, vmem, vmem),
        scratch_shapes=[
            pltpu.VMEM((shard,), f32),
            pltpu.VMEM((shard,), f32),
            pltpu.VMEM((n_out, 1, chunk * TILE), bf16),
            pltpu.VMEM((n_out, chunk, 8, 128), bf16),
            pltpu.VMEM((n_out, plane, span, 8, 128), bf16),
            pltpu.VMEM((n_out, span, 8, 128), f32),
            pltpu.VMEM((n_out, span, 8, 128), f32),
            pltpu.VMEM((span, 2, 8, 128), f32),
            pltpu.VMEM((2, 8, 128), f32),
            pltpu.VMEM((span, 8, 128), f32),
            pltpu.VMEM((1, 128), f32),
            pltpu.VMEM((n, 1, 128), f32),
            dma((n_out,)),
            dma((2,)),
            dma(()),
            dma((n_out, plane)),
            dma(()),
            dma((n_out,)),
            dma((2,)),
            dma(()),
            dma((n,)),
            dma(()),
            dma((n,)),
        ],
        compiler_params=pltpu.CompilerParams(
            collective_id=0, has_side_effects=True, vmem_limit_bytes=61 * 2**20
        ),
    )(grads, master, velocity, layer_offsets, layer_sizes, lars_skip)
    weights, nm, nv = pl.pallas_call(
        functools.partial(finish, (n, n_spa, shard, step, span)),
        out_shape=(
            jax.ShapeDtypeStruct((tiles, 8, 128), bf16),
            jax.ShapeDtypeStruct((shard,), f32),
            jax.ShapeDtypeStruct((shard,), f32),
        ),
        in_specs=[vmem, vmem, vmem],
        out_specs=(anywhere, anywhere, anywhere),
        scratch_shapes=[
            pltpu.VMEM((shard,), f32),
            pltpu.VMEM((shard,), f32),
            dma((n + 1,)),
            dma((2,)),
        ],
        compiler_params=pltpu.CompilerParams(vmem_limit_bytes=16 * 2**20),
    )(ags, nmw, nvw)
    return weights.reshape(params), nm, nv


def tiled(n_rep, n_spa, params):
    n = n_rep * n_spa
    shard = params // n
    n_in = math.isqrt(n_rep)
    rest = shard % TILE
    return (
        n_in * n_in == n_rep
        and n_in % 2 == 0
        and params % TILE == 0
        and shard >= TILE
        and 0 < n * rest <= TILE
        and rest <= 128
    )


def step_fn(n_rep, n_spa, grads, *rest):
    if tiled(n_rep, n_spa, grads.shape[2]):
        return windowed(n_rep, n_spa, grads, *rest)
    return shards(grads, *rest)


def shards(grads, master, velocity, layer_offsets, layer_sizes, lars_skip):
    n_rep = lax.axis_size("replica")
    n_spa = lax.axis_size("spatial")
    shard = master.shape[0]
    position = lax.axis_index(("replica", "spatial")) * shard + jnp.arange(shard, dtype=jnp.int32)
    inside = (position[None, :] >= layer_offsets[:, None]) & (
        position[None, :] < (layer_offsets + layer_sizes)[:, None]
    )
    onehot = inside.astype(jnp.float32)
    received = lax.all_to_all(
        grads[0, 0].reshape(n_rep, n_spa * shard),
        "replica",
        split_axis=0,
        concat_axis=0,
        tiled=True,
    )
    first = jnp.sum(received.astype(jnp.float32), axis=0)
    summed = lax.psum_scatter(
        first.reshape(n_spa, shard), "spatial", scatter_dimension=0, tiled=True
    )
    grad = summed.reshape(shard) / (n_rep * n_spa)
    gsq_local = jnp.dot(onehot, grad * grad, precision=lax.Precision.HIGHEST)
    wsq_local = jnp.dot(onehot, master * master, precision=lax.Precision.HIGHEST)
    wsq, gsq = lax.psum((wsq_local, gsq_local), ("replica", "spatial"))
    wnorm = jnp.sqrt(wsq)
    gnorm = jnp.sqrt(gsq)
    skipped = lars_skip.astype(jnp.float32)
    ratio = 0.02 * wnorm / (gnorm + 0.001 * wnorm + 1e-06)
    trust = skipped + (1.0 - skipped) * ratio
    decay = (1.0 - skipped) * 0.001
    trust_pos = jnp.dot(trust, onehot, precision=lax.Precision.HIGHEST)
    decay_pos = jnp.dot(decay, onehot, precision=lax.Precision.HIGHEST)
    new_velocity = 0.9 * velocity + 8.0 * trust_pos * (grad + decay_pos * master)
    new_master = master - new_velocity
    new_weights = lax.all_gather(
        new_master.astype(jnp.bfloat16), ("replica", "spatial"), axis=0, tiled=True
    )
    return (new_weights, new_master, new_velocity)


def solution(mesh):
    return jax.shard_map(
        functools.partial(step_fn, mesh.shape["replica"], mesh.shape["spatial"]),
        mesh=mesh,
        in_specs=(
            P("replica", "spatial", None),
            P(("replica", "spatial")),
            P(("replica", "spatial")),
            P(),
            P(),
            P(),
        ),
        out_specs=(P(), P(("replica", "spatial")), P(("replica", "spatial"))),
        check_vma=False,
    )
```
